32 devices in a mesh: slab: 2 (over x), py: 4 (over y, core), px: 4 (over z).
Axes of the slice: x: 2, y: 2, z: 4, core: 2. Of those that a mesh axis runs over, the one named last changes fastest.
Arguments:
- state: bfloat16 [2, 3, 16, 1024, 1024], P(None, None, 'slab', ('py', 'px')), may hold values from -12 to 12
- shells: int32 [16, 1024, 1024], P('slab', ('py', 'px')), may hold values from 0 to 511
Outputs:
- restored: float32 [2, 3, 16, 1024, 1024], P(None, None, ('slab', 'py'), None, 'px')
- spectrum: float32 [512], replicated
The draws below stay inside these ranges and needn't reach their ends.
All inputs are finite; a program needn't handle non-finite values.
Results may differ from the reference program's by a relative error of at most 0.0003.
Values may be sent and summed in bfloat16 or wider, within the bound.
A program may use at most 128 MiB of HBM per device.

```python
import math
import jax
import jax.numpy as jnp

X = 1024
Y = 1024
SHELLS = 512
Z = 16


def integer_root(squares):
    root = jnp.zeros_like(squares)
    for level in range(11, -1, -1):
        candidate = root + (1 << level)
        root = jnp.where(candidate * candidate <= squares, candidate, root)
    return root


def centred(count, key):
    spread = count // 8
    centre = count // 2 + jax.random.randint(key, (), -spread, spread + 1, jnp.int32)
    offsets = jnp.arange(count, dtype=jnp.int32) - centre
    reach = jnp.maximum(centre, count - 1 - centre)
    return (offsets, reach)


def shell_labels(key):
    base_key = jax.random.fold_in(key, 29)
    plane_key, row_key, column_key, jitter_key = jax.random.split(base_key, 4)
    plane_off, plane_reach = centred(Z, plane_key)
    row_off, row_reach = centred(Y, row_key)
    column_off, column_reach = centred(X, column_key)
    squares = (plane_off * plane_off)[:, None, None] + (row_off * row_off)[None, :, None] + (column_off * column_off)[None, None, :]
    radius = integer_root(squares)
    outer = integer_root(plane_reach * plane_reach + row_reach * row_reach + column_reach * column_reach)
    labels = radius * SHELLS // (outer + 1)
    jitter = jax.random.randint(jitter_key, (Z, Y, X), 0, 2, jnp.int32)
    return jnp.minimum(labels + jitter, SHELLS - 1).astype(jnp.int32)


def draw_shells(key, part):
    return shell_labels(key)


def draw_state(key, part):
    labels = shell_labels(key)
    first_key = jax.random.fold_in(jax.random.fold_in(key, 11), 0)
    column_key = jax.random.fold_in(jax.random.fold_in(key, 11), 2)
    row_key = jax.random.fold_in(jax.random.fold_in(key, 11), 3)
    decay = 1.0 / jnp.sqrt(1.0 + labels.astype(jnp.float32))
    column_gain = jnp.exp(jax.random.uniform(column_key, (X,), jnp.float32, math.log(0.5), math.log(2.0)))
    row_gain = jnp.exp(jax.random.uniform(row_key, (Y,), jnp.float32, math.log(0.7), math.log(1.4)))
    amplitude = decay * row_gain[None, :, None] * column_gain[None, None, :]
    base = jnp.clip(jax.random.normal(first_key, (2, 3, Z, Y, X), jnp.float32), -4.0, 4.0)
    return (base * amplitude[None, None, :, :, :]).astype(jnp.bfloat16)


def setup_inputs(seed: int = 0) -> dict:
    splits = jax.random.split(jax.random.key(seed), 3)
    state = draw_state(jax.random.fold_in(splits[2], 71), 0)
    shells = draw_shells(jax.random.fold_in(splits[2], 71), 0)
    return {"state": state, "shells": shells}


def reference(state, shells):
    restored = state.astype(jnp.float32)
    energy = 0.5 * jnp.sum(restored * restored, axis=(0, 1))
    totals = jax.ops.segment_sum(energy.reshape(-1), shells.reshape(-1).astype(jnp.int32), num_segments=SHELLS)
    spectrum = totals * (SHELLS / (Z * Y * X))
    return restored, spectrum
```

```python
import functools

import jax
import jax.numpy as jnp
from jax import lax
from jax.experimental import pallas as pl
from jax.experimental.pallas import tpu as pltpu
from jax.sharding import PartitionSpec as P

SHELLS = 512
LOW = 32
HIGH = SHELLS // LOW
LANES = 128
SPEC_ROWS = SHELLS // LANES
GROUP_ROWS = 16
CORES = 2
MESH = pl.DeviceIdType.MESH


def move_kernel(
    slab_count,
    py_count,
    px_count,
    state,
    shells,
    out,
    spec,
    moved,
    modes,
    labels,
    slab_parts,
    group_parts,
    state_sem,
    label_sem,
    send_sem,
    recv_sem,
    slab_send,
    slab_recv,
    part_send,
    part_recv,
    ready_sem,
    slab_ready,
):
    slab = lax.axis_index("slab")
    py = lax.axis_index("py")
    px = lax.axis_index("px")
    group = py_count * px_count
    me = py * px_count + px
    cores = CORES if py_count % CORES == 0 else 1
    _, _, planes, rows, columns = state.shape
    planes_out = planes // py_count
    columns_out = columns // px_count

    def position(any_py, any_px):
        return (cores - 1 - any_py % cores, any_py // cores, any_px)

    here = (cores - 1 - lax.rem(py, cores), py // cores, px)
    everyone = [(q_py, q_px) for q_py in range(py_count) for q_px in range(px_count)]

    def all_of(conditions):
        return functools.reduce(jnp.logical_and, conditions)

    def same(spot):
        return all_of([a == b for a, b in zip(spot, here)])

    def after_me(spot):
        return jnp.logical_and(
            all_of([a >= b for a, b in zip(spot, here)]), jnp.logical_not(same(spot))
        )

    def before_me(spot):
        return jnp.logical_and(
            all_of([a <= b for a, b in zip(spot, here)]), jnp.logical_not(same(spot))
        )

    def load_state(z):
        return pltpu.make_async_copy(state.at[:, :, z], modes.at[:, :, z], state_sem.at[z])

    def load_labels(z):
        return pltpu.make_async_copy(shells.at[z], labels.at[z], label_sem.at[z])

    def group_peer(step):
        peer = lax.rem(me + step, group)
        return (peer, peer // px_count, lax.rem(peer, px_count))

    def slab_peer(step):
        return lax.rem(slab + step, slab_count)

    def block(source, dest_py, dest_px):
        return source.at[
            :,
            :,
            pl.ds(dest_py * planes_out, planes_out),
            :,
            pl.ds(pl.multiple_of(dest_px * columns_out, columns_out), columns_out),
        ]

    def strip(buffer, source):
        return buffer.at[:, :, :, pl.ds(pl.multiple_of(source * rows, rows), rows), :]

    def send_block(dest_py, dest_px):
        return pltpu.make_async_remote_copy(
            src_ref=block(state, dest_py, dest_px),
            dst_ref=strip(moved, me),
            send_sem=send_sem.at[dest_py * px_count + dest_px],
            recv_sem=recv_sem.at[me],
            device_id=(slab, dest_py, dest_px),
            device_id_type=MESH,
        )

    def take_block(source, source_py, source_px):
        return pltpu.make_async_remote_copy(
            src_ref=block(state, source_py, source_px),
            dst_ref=strip(moved, source),
            send_sem=send_sem.at[source],
            recv_sem=recv_sem.at[source],
            device_id=(slab, source_py, source_px),
            device_id_type=MESH,
        )

    def slab_copy(dest, slot):
        return pltpu.make_async_remote_copy(
            src_ref=slab_parts.at[slab],
            dst_ref=slab_parts.at[slot],
            send_sem=slab_send.at[dest],
            recv_sem=slab_recv.at[slot],
            device_id=(dest, py, px),
            device_id_type=MESH,
        )

    def part_copy(dest, dest_py, dest_px, slot):
        return pltpu.make_async_remote_copy(
            src_ref=group_parts.at[me],
            dst_ref=group_parts.at[slot],
            send_sem=part_send.at[dest],
            recv_sem=part_recv.at[slot],
            device_id=(slab, dest_py, dest_px),
            device_id_type=MESH,
        )

    barrier = pltpu.get_barrier_semaphore()
    for q_py, q_px in everyone:

        @pl.when(after_me(position(q_py, q_px)))
        def _():
            pl.semaphore_signal(
                barrier, inc=1, device_id=(slab, q_py, q_px), device_id_type=MESH
            )

    for q_slab in range(1, slab_count):

        @pl.when(q_slab > slab)
        def _():
            pl.semaphore_signal(
                barrier, inc=1, device_id=(q_slab, py, px), device_id_type=MESH
            )

    before = (here[0] + 1) * (here[1] + 1) * (here[2] + 1) - 1 + slab

    @pl.when(before > 0)
    def _():
        pl.semaphore_wait(barrier, before)

    def spot_of(dest_py, dest_px):
        return (cores - 1 - lax.rem(dest_py, cores), dest_py // cores, dest_px)

    def send_if(condition, dest_py, dest_px):
        @pl.when(condition)
        def _():
            send_block(dest_py, dest_px).start()

    def send_far(wanted):
        for distance in range(px_count - 1, 1, -1):
            for turn in range(py_count):
                dest_py = lax.rem(py + turn, py_count)
                for dest_px in (px + distance, px - distance):
                    inside = jnp.logical_and(dest_px >= 0, dest_px < px_count)
                    send_if(
                        jnp.logical_and(inside, wanted(spot_of(dest_py, dest_px))),
                        dest_py,
                        dest_px,
                    )

    def send_near():
        for turn in range(py_count):
            dest_py = lax.rem(py + turn, py_count)
            send_if(px - 1 >= 0, dest_py, px - 1)
            if turn > 0:
                send_if(px + 1 < px_count, dest_py, px + 1)
        for turn in range(1, py_count):
            send_block(lax.rem(py + turn, py_count), px).start()

    def hear(wanted):
        for q_py, q_px in everyone:
            spot = position(q_py, q_px)

            @pl.when(jnp.logical_and(after_me(spot), wanted(q_py, q_px)))
            def _():
                pl.semaphore_wait(ready_sem.at[q_py * px_count + q_px], 1)

    send_far(before_me)

    for q_py, q_px in everyone:

        @pl.when(before_me(position(q_py, q_px)))
        def _():
            pl.semaphore_signal(
                ready_sem.at[me], inc=1, device_id=(slab, q_py, q_px), device_id_type=MESH
            )

    for q_slab in range(slab_count - 1):

        @pl.when(q_slab < slab)
        def _():
            pl.semaphore_signal(
                slab_ready.at[slab], inc=1, device_id=(q_slab, py, px), device_id_type=MESH
            )

    def is_next(q_py, q_px):
        return jnp.logical_and(q_py == py, q_px == px + 1)

    hear(is_next)
    send_if(px + 1 < px_count, py, px + 1)
    hear(lambda q_py, q_px: jnp.logical_not(is_next(q_py, q_px)))
    send_far(lambda spot: jnp.logical_not(before_me(spot)))

    for z in range(planes):
        load_state(z).start()
        load_labels(z).start()

    low_ids = lax.broadcasted_iota(jnp.int32, (LOW, columns), 0)
    high_ids = lax.broadcasted_iota(jnp.int32, (HIGH, columns), 0)

    def add_rows(z, start, running):
        values = modes[:, :, z, pl.ds(start, GROUP_ROWS), :].astype(jnp.float32)
        energy = 0.5 * jnp.sum(values * values, axis=(0, 1))
        upper = energy.astype(jnp.bfloat16).astype(jnp.float32)
        lower = energy - upper
        numbers = labels[z, pl.ds(start, GROUP_ROWS), :]
        high = numbers >> (LOW.bit_length() - 1)
        low = numbers & (LOW - 1)
        for row in range(GROUP_ROWS):
            one = slice(row, row + 1)
            hot = high_ids == high[one]
            weighted = jnp.concatenate(
                [jnp.where(hot, upper[one], 0.0), jnp.where(hot, lower[one], 0.0)], axis=0
            ).astype(jnp.bfloat16)
            onehot = jnp.where(low_ids == low[one], 1.0, 0.0).astype(jnp.bfloat16)
            running = running + lax.dot_general(
                weighted, onehot, (((1,), (1,)), ((), ())), preferred_element_type=jnp.float32
            )
        return running

    running = jnp.zeros((2 * HIGH, LOW), jnp.float32)
    for z in range(planes):
        load_state(z).wait()
        load_labels(z).wait()

    groups = rows // GROUP_ROWS
    running = lax.fori_loop(
        0,
        planes * groups,
        lambda i, total: add_rows(
            i // groups, pl.multiple_of(lax.rem(i, groups) * GROUP_ROWS, GROUP_ROWS), total
        ),
        running,
    )
    part = running[:HIGH] + running[HIGH:]
    per_row = LANES // LOW
    for high in range(HIGH):
        lane = (high % per_row) * LOW
        slab_parts[slab, high // per_row : high // per_row + 1, lane : lane + LOW] = part[
            high : high + 1
        ]

    for q_slab in range(1, slab_count):

        @pl.when(q_slab > slab)
        def _():
            pl.semaphore_wait(slab_ready.at[q_slab], 1)

    for step in range(1, slab_count):
        slab_copy(slab_peer(step), slab).start()
    for step in range(1, slab_count):
        slab_copy(slab_peer(step), slab_peer(step)).wait_recv()
    total = slab_parts[0]
    for slot in range(1, slab_count):
        total = total + slab_parts[slot]
    group_parts[me] = total
    for step in range(1, group):
        part_copy(*group_peer(step), me).start()

    send_near()

    def widen(source, target):
        for real in range(source.shape[0]):
            for part_of in range(source.shape[1]):
                for plane in range(source.shape[2]):
                    target[real, part_of, plane] = source[real, part_of, plane].astype(
                        jnp.float32
                    )

    widen(block(modes, py, px), strip(out, me))

    for step in range(1, group):
        peer, peer_py, peer_px = group_peer(step)
        part_copy(peer, peer_py, peer_px, peer).wait_recv()
    total = group_parts[0]
    for slot in range(1, group):
        total = total + group_parts[slot]
    modes_all = planes * rows * columns * slab_count * group
    spec[...] = total * (SHELLS / modes_all)

    def take_and_widen(source_py, source_px):
        source = source_py * px_count + source_px
        take_block(source, source_py, source_px).wait_recv()
        widen(strip(moved, source), strip(out, source))

    for step in range(1, slab_count):
        slab_copy(slab_peer(step), slab).wait_send()
    for step in range(1, group):
        peer, peer_py, peer_px = group_peer(step)
        part_copy(peer, peer_py, peer_px, me).wait_send()

    half = px_count // 2
    ahead = jnp.where(px < half, 1, px_count - 1)

    def take_step(step, carry):
        source_px = lax.rem(px + ahead * (half + step // py_count), px_count)
        source_py = lax.rem(py + py_count - lax.rem(step, py_count), py_count)

        @pl.when(jnp.logical_or(source_px != px, source_py != py))
        def _():
            take_and_widen(source_py, source_px)

        return carry

    lax.fori_loop(0, group, take_step, 0)
    for step in range(1, group):
        _, peer_py, peer_px = group_peer(step)
        send_block(peer_py, peer_px).wait_send()


def store_kernel(widened, totals, out, spectrum, out_sem, spectrum_sem):
    pieces = [
        (real, part, plane)
        for real in range(widened.shape[0])
        for part in range(widened.shape[1])
        for plane in range(widened.shape[2])
    ]
    copies = [
        pltpu.make_async_copy(widened.at[piece], out.at[piece], out_sem.at[i])
        for i, piece in enumerate(pieces)
    ]
    copies.append(pltpu.make_async_copy(totals, spectrum, spectrum_sem))
    for copy in copies:
        copy.start()
    for copy in copies:
        copy.wait()


def local(state, shells):
    slab_count = lax.axis_size("slab")
    py_count = lax.axis_size("py")
    px_count = lax.axis_size("px")
    group = py_count * px_count
    _, _, planes, rows, columns = state.shape
    moved_shape = (2, 3, planes // py_count, rows * group, columns // px_count)
    widened, totals = pl.pallas_call(
        functools.partial(move_kernel, slab_count, py_count, px_count),
        out_shape=(
            pltpu.VMEM(moved_shape, jnp.float32),
            pltpu.VMEM((SPEC_ROWS, LANES), jnp.float32),
        ),
        in_specs=[pl.BlockSpec(memory_space=pl.ANY)] * 2,
        out_specs=(
            pl.BlockSpec(memory_space=pltpu.VMEM),
            pl.BlockSpec(memory_space=pltpu.VMEM),
        ),
        scratch_shapes=[
            pltpu.VMEM(moved_shape, state.dtype),
            pltpu.VMEM(state.shape, state.dtype),
            pltpu.VMEM(shells.shape, shells.dtype),
            pltpu.VMEM((slab_count, SPEC_ROWS, LANES), jnp.float32),
            pltpu.VMEM((group, SPEC_ROWS, LANES), jnp.float32),
            pltpu.SemaphoreType.DMA((planes,)),
            pltpu.SemaphoreType.DMA((planes,)),
            pltpu.SemaphoreType.DMA((group,)),
            pltpu.SemaphoreType.DMA((group,)),
            pltpu.SemaphoreType.DMA((slab_count,)),
            pltpu.SemaphoreType.DMA((slab_count,)),
            pltpu.SemaphoreType.DMA((group,)),
            pltpu.SemaphoreType.DMA((group,)),
            pltpu.SemaphoreType.REGULAR((group,)),
            pltpu.SemaphoreType.REGULAR((slab_count,)),
        ],
        name="move",
        compiler_params=pltpu.CompilerParams(
            collective_id=0, has_side_effects=True, vmem_limit_bytes=40 << 20
        ),
    )(
        pltpu.with_memory_space_constraint(state, pltpu.HBM),
        pltpu.with_memory_space_constraint(shells, pltpu.HBM),
    )
    restored, spectrum = pl.pallas_call(
        store_kernel,
        out_shape=(
            jax.ShapeDtypeStruct(moved_shape, jnp.float32),
            jax.ShapeDtypeStruct((SPEC_ROWS, LANES), jnp.float32),
        ),
        in_specs=[pl.BlockSpec(memory_space=pltpu.VMEM)] * 2,
        out_specs=(
            pl.BlockSpec(memory_space=pl.ANY),
            pl.BlockSpec(memory_space=pl.ANY),
        ),
        scratch_shapes=[
            pltpu.SemaphoreType.DMA((2 * 3 * (planes // py_count),)),
            pltpu.SemaphoreType.DMA,
        ],
        name="store",
        compiler_params=pltpu.CompilerParams(vmem_limit_bytes=40 << 20),
    )(widened, totals)
    return (restored, spectrum.reshape(SHELLS))


def solution(mesh):
    return jax.shard_map(
        local,
        mesh=mesh,
        in_specs=(P(None, None, "slab", ("py", "px"), None), P("slab", ("py", "px"), None)),
        out_specs=(P(None, None, ("slab", "py"), None, "px"), P()),
        check_vma=False,
    )
```

```python
import functools

import jax
import jax.numpy as jnp
from jax import lax
from jax.experimental import pallas as pl
from jax.experimental.pallas import tpu as pltpu
from jax.sharding import PartitionSpec as P

SHELLS = 512
LOW = 32
HIGH = SHELLS // LOW
LANES = 128
SPEC_ROWS = SHELLS // LANES
GROUP_ROWS = 16
CORES = 2
MESH = pl.DeviceIdType.MESH


def core_count(py_count):
    return CORES if py_count % CORES == 0 else 1


def inner_at(px, px_count):
    half = px_count // 2
    return jnp.logical_and(half > 0, jnp.logical_or(px == half - 1, px == half))


def across(px, px_count):
    return 2 * (px_count // 2) - 1 - px


def is_late(py_count, px_count, py, px, dest_py, dest_px):
    cores = core_count(py_count)
    lasts = jnp.logical_and(lax.rem(py, cores) == cores - 1, lax.rem(dest_py, cores) == cores - 1)
    mates = jnp.logical_and(inner_at(px, px_count), dest_px == across(px, px_count))
    return jnp.logical_and(cores > 1, jnp.logical_and(lasts, mates))


def swap_kernel(py_count, px_count, state, after, rest, moved, send_sem, recv_sem):
    slab = lax.axis_index("slab")
    py = lax.axis_index("py")
    px = lax.axis_index("px")
    cores = core_count(py_count)
    chips = py_count // cores
    _, _, planes, rows, columns = state.shape
    planes_out = planes // py_count
    columns_out = columns // px_count
    mate = across(px, px_count)

    def copy(chip, slot):
        return pltpu.make_async_remote_copy(
            src_ref=state.at[
                :,
                :,
                pl.ds((chip * cores + cores - 1) * planes_out, planes_out),
                :,
                pl.ds(pl.multiple_of(mate * columns_out, columns_out), columns_out),
            ],
            dst_ref=moved.at[slot],
            send_sem=send_sem.at[chip],
            recv_sem=recv_sem.at[slot],
            device_id=(slab, chip * cores + cores - 1, mate),
            device_id_type=MESH,
        )

    @pl.when(is_late(py_count, px_count, py, px, cores - 1, mate))
    def _():
        here = py // cores
        barrier = pltpu.get_barrier_semaphore()
        for chip in range(chips):
            pl.semaphore_signal(
                barrier, inc=1, device_id=(slab, chip * cores + cores - 1, mate), device_id_type=MESH
            )
        pl.semaphore_wait(barrier, chips)
        for turn in range(chips):
            copy(lax.rem(here + turn, chips), here).start()
        for turn in range(chips):
            chip = lax.rem(here + chips - turn, chips)
            copy(chip, chip).wait_recv()
            for real in range(moved.shape[1]):
                for part in range(moved.shape[2]):
                    for plane in range(planes_out):
                        piece = (chip, real, part, plane)
                        rest[piece] = moved[piece].astype(jnp.float32)
        for chip in range(chips):
            copy(chip, here).wait_send()


def move_kernel(
    slab_count,
    py_count,
    px_count,
    state,
    shells,
    out,
    spec,
    moved,
    modes,
    labels,
    slab_parts,
    group_parts,
    state_sem,
    label_sem,
    send_sem,
    recv_sem,
    slab_send,
    slab_recv,
    part_send,
    part_recv,
    ready_sem,
    slab_ready,
):
    slab = lax.axis_index("slab")
    py = lax.axis_index("py")
    px = lax.axis_index("px")
    group = py_count * px_count
    me = py * px_count + px
    cores = core_count(py_count)
    _, _, planes, rows, columns = state.shape
    planes_out = planes // py_count
    columns_out = columns // px_count

    def position(any_py, any_px):
        return (cores - 1 - any_py % cores, any_py // cores, any_px)

    here = (cores - 1 - lax.rem(py, cores), py // cores, px)
    everyone = [(q_py, q_px) for q_py in range(py_count) for q_px in range(px_count)]

    def all_of(conditions):
        return functools.reduce(jnp.logical_and, conditions)

    def same(spot):
        return all_of([a == b for a, b in zip(spot, here)])

    def after_me(spot):
        return jnp.logical_and(
            all_of([a >= b for a, b in zip(spot, here)]), jnp.logical_not(same(spot))
        )

    def before_me(spot):
        return jnp.logical_and(
            all_of([a <= b for a, b in zip(spot, here)]), jnp.logical_not(same(spot))
        )

    def load_state(z):
        return pltpu.make_async_copy(state.at[:, :, z], modes.at[:, :, z], state_sem.at[z])

    def load_labels(z):
        return pltpu.make_async_copy(shells.at[z], labels.at[z], label_sem.at[z])

    def group_peer(step):
        peer = lax.rem(me + step, group)
        return (peer, peer // px_count, lax.rem(peer, px_count))

    def slab_peer(step):
        return lax.rem(slab + step, slab_count)

    def block(source, dest_py, dest_px):
        return source.at[
            :,
            :,
            pl.ds(dest_py * planes_out, planes_out),
            :,
            pl.ds(pl.multiple_of(dest_px * columns_out, columns_out), columns_out),
        ]

    def strip(buffer, source):
        return buffer.at[:, :, :, pl.ds(pl.multiple_of(source * rows, rows), rows), :]

    def send_block(dest_py, dest_px):
        return pltpu.make_async_remote_copy(
            src_ref=block(state, dest_py, dest_px),
            dst_ref=strip(moved, me),
            send_sem=send_sem.at[dest_py * px_count + dest_px],
            recv_sem=recv_sem.at[me],
            device_id=(slab, dest_py, dest_px),
            device_id_type=MESH,
        )

    def take_block(source, source_py, source_px):
        return pltpu.make_async_remote_copy(
            src_ref=block(state, source_py, source_px),
            dst_ref=strip(moved, source),
            send_sem=send_sem.at[source],
            recv_sem=recv_sem.at[source],
            device_id=(slab, source_py, source_px),
            device_id_type=MESH,
        )

    def slab_copy(dest, slot):
        return pltpu.make_async_remote_copy(
            src_ref=slab_parts.at[slab],
            dst_ref=slab_parts.at[slot],
            send_sem=slab_send.at[dest],
            recv_sem=slab_recv.at[slot],
            device_id=(dest, py, px),
            device_id_type=MESH,
        )

    def part_copy(dest, dest_py, dest_px, slot):
        return pltpu.make_async_remote_copy(
            src_ref=group_parts.at[me],
            dst_ref=group_parts.at[slot],
            send_sem=part_send.at[dest],
            recv_sem=part_recv.at[slot],
            device_id=(slab, dest_py, dest_px),
            device_id_type=MESH,
        )

    barrier = pltpu.get_barrier_semaphore()
    for q_py, q_px in everyone:

        @pl.when(after_me(position(q_py, q_px)))
        def _():
            pl.semaphore_signal(
                barrier, inc=1, device_id=(slab, q_py, q_px), device_id_type=MESH
            )

    for q_slab in range(1, slab_count):

        @pl.when(q_slab > slab)
        def _():
            pl.semaphore_signal(
                barrier, inc=1, device_id=(q_slab, py, px), device_id_type=MESH
            )

    before = (here[0] + 1) * (here[1] + 1) * (here[2] + 1) - 1 + slab

    @pl.when(before > 0)
    def _():
        pl.semaphore_wait(barrier, before)

    def spot_of(dest_py, dest_px):
        return (cores - 1 - lax.rem(dest_py, cores), dest_py // cores, dest_px)

    def late(dest_py, dest_px):
        return is_late(py_count, px_count, py, px, dest_py, dest_px)

    def send_if(condition, dest_py, dest_px):
        @pl.when(jnp.logical_and(condition, jnp.logical_not(late(dest_py, dest_px))))
        def _():
            send_block(dest_py, dest_px).start()

    def send_at(distance, wanted, turns=range(py_count)):
        for turn in turns:
            dest_py = lax.rem(py + turn, py_count)
            for dest_px in (px + distance, px - distance):
                inside = jnp.logical_and(dest_px >= 0, dest_px < px_count)
                send_if(
                    jnp.logical_and(inside, wanted(dest_py, dest_px)), dest_py, dest_px
                )

    def send_far(wanted):
        for distance in range(px_count - 1, 1, -1):
            send_at(distance, wanted)

    next_py = py + cores - 1 - 2 * lax.rem(py, cores)

    def is_next(q_py, q_px):
        return all_of([q_py == next_py, q_px == px + 1, q_px == px_count // 2])

    def send_near():
        apart = [turn for turn in range(py_count) if turn % cores]
        alike = [turn for turn in range(py_count) if turn % cores == 0]
        send_at(1, lambda *dest: jnp.logical_not(is_next(*dest)), apart + alike)
        for turn in range(1, py_count):
            send_block(lax.rem(py + turn, py_count), px).start()

    def hear(rise_y, rise_px):
        for core in range(cores):
            spot = (core, here[1] + rise_y, px + rise_px)
            q_py = spot[1] * cores + cores - 1 - core
            exists = jnp.logical_and(q_py < py_count, spot[2] < px_count)

            @pl.when(jnp.logical_and(exists, after_me(spot)))
            def _():
                pl.semaphore_wait(ready_sem.at[q_py * px_count + spot[2]], 1)

    for q_py, q_px in everyone:

        @pl.when(before_me(position(q_py, q_px)))
        def _():
            pl.semaphore_signal(
                ready_sem.at[me], inc=1, device_id=(slab, q_py, q_px), device_id_type=MESH
            )

    send_far(lambda *dest: before_me(spot_of(*dest)))

    for q_slab in range(slab_count - 1):

        @pl.when(q_slab < slab)
        def _():
            pl.semaphore_signal(
                slab_ready.at[slab], inc=1, device_id=(q_slab, py, px), device_id_type=MESH
            )

    rises = [(y, x) for y in range(py_count // cores) for x in range(px_count)]
    for rise_y, rise_px in sorted(rises, key=lambda rise: (sum(rise), rise[0])):
        hear(rise_y, rise_px)

        def reached(dest_py, dest_px):
            return all_of(
                [
                    jnp.maximum(dest_py // cores - here[1], 0) == rise_y,
                    jnp.maximum(dest_px - px, 0) == rise_px,
                    jnp.logical_not(before_me(spot_of(dest_py, dest_px))),
                ]
            )

        if rise_px == 1 and rise_y == 0:
            send_if(is_next(next_py, px + 1), next_py, px + 1)
        send_far(reached)

    for z in range(planes):
        load_state(z).start()
        load_labels(z).start()

    low_ids = lax.broadcasted_iota(jnp.int32, (LOW, columns), 0)
    high_ids = lax.broadcasted_iota(jnp.int32, (HIGH, columns), 0)

    def add_rows(z, start, running):
        values = modes[:, :, z, pl.ds(start, GROUP_ROWS), :].astype(jnp.float32)
        energy = 0.5 * jnp.sum(values * values, axis=(0, 1))
        upper = energy.astype(jnp.bfloat16).astype(jnp.float32)
        lower = energy - upper
        numbers = labels[z, pl.ds(start, GROUP_ROWS), :]
        high = numbers >> (LOW.bit_length() - 1)
        low = numbers & (LOW - 1)
        for row in range(GROUP_ROWS):
            one = slice(row, row + 1)
            hot = high_ids == high[one]
            weighted = jnp.concatenate(
                [jnp.where(hot, upper[one], 0.0), jnp.where(hot, lower[one], 0.0)], axis=0
            ).astype(jnp.bfloat16)
            onehot = jnp.where(low_ids == low[one], 1.0, 0.0).astype(jnp.bfloat16)
            running = running + lax.dot_general(
                weighted, onehot, (((1,), (1,)), ((), ())), preferred_element_type=jnp.float32
            )
        return running

    running = jnp.zeros((2 * HIGH, LOW), jnp.float32)
    for z in range(planes):
        load_state(z).wait()
        load_labels(z).wait()

    groups = rows // GROUP_ROWS
    running = lax.fori_loop(
        0,
        planes * groups,
        lambda i, total: add_rows(
            i // groups, pl.multiple_of(lax.rem(i, groups) * GROUP_ROWS, GROUP_ROWS), total
        ),
        running,
    )
    part = running[:HIGH] + running[HIGH:]
    per_row = LANES // LOW
    for high in range(HIGH):
        lane = (high % per_row) * LOW
        slab_parts[slab, high // per_row : high // per_row + 1, lane : lane + LOW] = part[
            high : high + 1
        ]

    for q_slab in range(1, slab_count):

        @pl.when(q_slab > slab)
        def _():
            pl.semaphore_wait(slab_ready.at[q_slab], 1)

    for step in range(1, slab_count):
        slab_copy(slab_peer(step), slab).start()
    for step in range(1, slab_count):
        slab_copy(slab_peer(step), slab_peer(step)).wait_recv()
    total = slab_parts[0]
    for slot in range(1, slab_count):
        total = total + slab_parts[slot]
    group_parts[me] = total
    for step in range(1, group):
        part_copy(*group_peer(step), me).start()

    send_near()

    def widen(source, target):
        for real in range(source.shape[0]):
            for part_of in range(source.shape[1]):
                for plane in range(source.shape[2]):
                    target[real, part_of, plane] = source[real, part_of, plane].astype(
                        jnp.float32
                    )

    widen(block(modes, py, px), strip(out, me))

    for step in range(1, group):
        peer, peer_py, peer_px = group_peer(step)
        part_copy(peer, peer_py, peer_px, peer).wait_recv()
    total = group_parts[0]
    for slot in range(1, group):
        total = total + group_parts[slot]
    modes_all = planes * rows * columns * slab_count * group
    spec[...] = total * (SHELLS / modes_all)

    def take_and_widen(source_py, source_px):
        source = source_py * px_count + source_px
        take_block(source, source_py, source_px).wait_recv()
        widen(strip(moved, source), strip(out, source))

    for step in range(1, slab_count):
        slab_copy(slab_peer(step), slab).wait_send()
    for step in range(1, group):
        peer, peer_py, peer_px = group_peer(step)
        part_copy(peer, peer_py, peer_px, me).wait_send()

    half = px_count // 2
    ahead = jnp.where(px < half, 1, px_count - 1)

    def take_step(step, carry):
        source_px = lax.rem(px + ahead * (half + step // py_count), px_count)
        source_py = lax.rem(py + py_count - lax.rem(step, py_count), py_count)

        other = jnp.logical_or(source_px != px, source_py != py)
        here_now = jnp.logical_not(late(source_py, source_px))

        @pl.when(jnp.logical_and(other, here_now))
        def _():
            take_and_widen(source_py, source_px)

        return carry

    lax.fori_loop(0, group, take_step, 0)
    for step in range(1, group):
        _, peer_py, peer_px = group_peer(step)

        @pl.when(jnp.logical_not(late(peer_py, peer_px)))
        def _():
            send_block(peer_py, peer_px).wait_send()


def run_copies(copies, sems):
    def each(act):
        for i, (condition, source, target) in enumerate(copies):
            copy = pltpu.make_async_copy(source, target, sems.at[i])
            if condition is None:
                act(copy)
            else:
                pl.when(condition)(functools.partial(act, copy))

    each(lambda copy: copy.start())
    each(lambda copy: copy.wait())


def store_kernel(py_count, px_count, widened, totals, out, spectrum, sems):
    py = lax.axis_index("py")
    px = lax.axis_index("px")
    rows = out.shape[3] // (py_count * px_count)
    copies = [(None, totals, spectrum)]
    for source_py in range(py_count):
        for source_px in range(px_count):
            start = (source_py * px_count + source_px) * rows
            strip = (slice(None), slice(None), slice(None), pl.ds(start, rows))
            missing = is_late(py_count, px_count, py, px, source_py, source_px)
            copies.append((jnp.logical_not(missing), widened.at[strip], out.at[strip]))
    run_copies(copies, sems)


def rest_kernel(py_count, px_count, rest, stored, out, sems):
    py = lax.axis_index("py")
    px = lax.axis_index("px")
    cores = core_count(py_count)
    rows = rest.shape[4]
    mate = across(px, px_count)
    copies = []
    for chip in range(py_count // cores):
        start = pl.multiple_of(((chip * cores + cores - 1) * px_count + mate) * rows, rows)
        copies.append(
            (
                is_late(py_count, px_count, py, px, chip * cores + cores - 1, mate),
                rest.at[chip],
                out.at[:, :, :, pl.ds(start, rows)],
            )
        )
    run_copies(copies, sems)


def local(state, shells):
    slab_count = lax.axis_size("slab")
    py_count = lax.axis_size("py")
    px_count = lax.axis_size("px")
    group = py_count * px_count
    _, _, planes, rows, columns = state.shape
    moved_shape = (2, 3, planes // py_count, rows * group, columns // px_count)
    widened, totals = pl.pallas_call(
        functools.partial(move_kernel, slab_count, py_count, px_count),
        out_shape=(
            pltpu.VMEM(moved_shape, jnp.float32),
            pltpu.VMEM((SPEC_ROWS, LANES), jnp.float32),
        ),
        in_specs=[pl.BlockSpec(memory_space=pl.ANY)] * 2,
        out_specs=(
            pl.BlockSpec(memory_space=pltpu.VMEM),
            pl.BlockSpec(memory_space=pltpu.VMEM),
        ),
        scratch_shapes=[
            pltpu.VMEM(moved_shape, state.dtype),
            pltpu.VMEM(state.shape, state.dtype),
            pltpu.VMEM(shells.shape, shells.dtype),
            pltpu.VMEM((slab_count, SPEC_ROWS, LANES), jnp.float32),
            pltpu.VMEM((group, SPEC_ROWS, LANES), jnp.float32),
            pltpu.SemaphoreType.DMA((planes,)),
            pltpu.SemaphoreType.DMA((planes,)),
            pltpu.SemaphoreType.DMA((group,)),
            pltpu.SemaphoreType.DMA((group,)),
            pltpu.SemaphoreType.DMA((slab_count,)),
            pltpu.SemaphoreType.DMA((slab_count,)),
            pltpu.SemaphoreType.DMA((group,)),
            pltpu.SemaphoreType.DMA((group,)),
            pltpu.SemaphoreType.REGULAR((group,)),
            pltpu.SemaphoreType.REGULAR((slab_count,)),
        ],
        name="move",
        compiler_params=pltpu.CompilerParams(
            collective_id=0, has_side_effects=True, vmem_limit_bytes=40 << 20
        ),
    )(
        pltpu.with_memory_space_constraint(state, pltpu.HBM),
        pltpu.with_memory_space_constraint(shells, pltpu.HBM),
    )
    anywhere = pl.BlockSpec(memory_space=pl.ANY)
    in_vmem = pl.BlockSpec(memory_space=pltpu.VMEM)
    stored, spectrum = pl.pallas_call(
        functools.partial(store_kernel, py_count, px_count),
        out_shape=(
            jax.ShapeDtypeStruct(moved_shape, jnp.float32),
            jax.ShapeDtypeStruct((SPEC_ROWS, LANES), jnp.float32),
        ),
        in_specs=[in_vmem] * 2,
        out_specs=(anywhere, anywhere),
        scratch_shapes=[pltpu.SemaphoreType.DMA((1 + group,))],
        name="store",
        compiler_params=pltpu.CompilerParams(vmem_limit_bytes=40 << 20),
    )(widened, totals)
    chips = py_count // core_count(py_count)
    rest_shape = (chips, 2, 3, planes // py_count, rows, columns // px_count)
    rest = pl.pallas_call(
        functools.partial(swap_kernel, py_count, px_count),
        out_shape=pltpu.VMEM(rest_shape, jnp.float32),
        in_specs=[anywhere] * 2,
        out_specs=in_vmem,
        scratch_shapes=[
            pltpu.VMEM(rest_shape, state.dtype),
            pltpu.SemaphoreType.DMA((chips,)),
            pltpu.SemaphoreType.DMA((chips,)),
        ],
        name="swap",
        compiler_params=pltpu.CompilerParams(
            collective_id=1, has_side_effects=True, vmem_limit_bytes=40 << 20
        ),
    )(
        pltpu.with_memory_space_constraint(state, pltpu.HBM),
        pltpu.with_memory_space_constraint(spectrum, pltpu.HBM),
    )
    restored = pl.pallas_call(
        functools.partial(rest_kernel, py_count, px_count),
        out_shape=jax.ShapeDtypeStruct(moved_shape, jnp.float32),
        in_specs=[in_vmem, anywhere],
        out_specs=anywhere,
        scratch_shapes=[pltpu.SemaphoreType.DMA((chips,))],
        input_output_aliases={1: 0},
        name="store_rest",
        compiler_params=pltpu.CompilerParams(vmem_limit_bytes=40 << 20),
    )(rest, stored)
    return (restored, spectrum.reshape(SHELLS))


def solution(mesh):
    return jax.shard_map(
        local,
        mesh=mesh,
        in_specs=(P(None, None, "slab", ("py", "px"), None), P("slab", ("py", "px"), None)),
        out_specs=(P(None, None, ("slab", "py"), None, "px"), P()),
        check_vma=False,
    )
```

```python
import functools

import jax
import jax.numpy as jnp
from jax import lax
from jax.experimental import pallas as pl
from jax.experimental.pallas import tpu as pltpu
from jax.sharding import PartitionSpec as P

SHELLS = 512
LOW = 32
HIGH = SHELLS // LOW
LANES = 128
SPEC_ROWS = SHELLS // LANES
GROUP_ROWS = 16
CORES = 2
MESH = pl.DeviceIdType.MESH


def core_count(py_count):
    return CORES if py_count % CORES == 0 else 1


def inner_at(px, px_count):
    half = px_count // 2
    return jnp.logical_and(half > 0, jnp.logical_or(px == half - 1, px == half))


def across(px, px_count):
    return 2 * (px_count // 2) - 1 - px


def is_late(py_count, px_count, py, px, dest_py, dest_px):
    cores = core_count(py_count)
    lasts = jnp.logical_and(lax.rem(py, cores) == cores - 1, lax.rem(dest_py, cores) == cores - 1)
    mates = jnp.logical_and(inner_at(px, px_count), dest_px == across(px, px_count))
    return jnp.logical_and(cores > 1, jnp.logical_and(lasts, mates))


def swap_kernel(py_count, px_count, state, after, rest, moved, send_sem, recv_sem):
    slab = lax.axis_index("slab")
    py = lax.axis_index("py")
    px = lax.axis_index("px")
    cores = core_count(py_count)
    chips = py_count // cores
    _, _, planes, rows, columns = state.shape
    planes_out = planes // py_count
    columns_out = columns // px_count
    mate = across(px, px_count)

    def copy(chip, slot):
        return pltpu.make_async_remote_copy(
            src_ref=state.at[
                :,
                :,
                pl.ds((chip * cores + cores - 1) * planes_out, planes_out),
                :,
                pl.ds(pl.multiple_of(mate * columns_out, columns_out), columns_out),
            ],
            dst_ref=moved.at[slot],
            send_sem=send_sem.at[chip],
            recv_sem=recv_sem.at[slot],
            device_id=(slab, chip * cores + cores - 1, mate),
            device_id_type=MESH,
        )

    @pl.when(is_late(py_count, px_count, py, px, cores - 1, mate))
    def _():
        here = py // cores
        barrier = pltpu.get_barrier_semaphore()
        for chip in range(chips):
            pl.semaphore_signal(
                barrier, inc=1, device_id=(slab, chip * cores + cores - 1, mate), device_id_type=MESH
            )
        pl.semaphore_wait(barrier, chips)
        for turn in range(chips):
            copy(turn, here).start()
        for turn in range(chips):
            chip = lax.rem(here + chips - turn, chips)
            copy(chip, chip).wait_recv()
            for real in range(moved.shape[1]):
                for part in range(moved.shape[2]):
                    for plane in range(planes_out):
                        piece = (chip, real, part, plane)
                        rest[piece] = moved[piece].astype(jnp.float32)
        for chip in range(chips):
            copy(chip, here).wait_send()


def move_kernel(
    slab_count,
    py_count,
    px_count,
    state,
    shells,
    out,
    spec,
    moved,
    modes,
    labels,
    slab_parts,
    group_parts,
    state_sem,
    label_sem,
    send_sem,
    recv_sem,
    slab_send,
    slab_recv,
    part_send,
    part_recv,
    ready_sem,
    slab_ready,
):
    slab = lax.axis_index("slab")
    py = lax.axis_index("py")
    px = lax.axis_index("px")
    group = py_count * px_count
    me = py * px_count + px
    cores = core_count(py_count)
    _, _, planes, rows, columns = state.shape
    planes_out = planes // py_count
    columns_out = columns // px_count

    def position(any_py, any_px):
        return (cores - 1 - any_py % cores, any_py // cores, any_px)

    here = (cores - 1 - lax.rem(py, cores), py // cores, px)
    sizes = (cores, py_count // cores, px_count)
    offsets = sorted(
        (
            (core, y, x)
            for core in range(sizes[0])
            for y in range(sizes[1])
            for x in range(sizes[2])
            if core + y + x > 0
        ),
        key=lambda offset: (offset[1] + offset[2], offset[1], offset[0]),
    )

    def tell_all(way, semaphore):
        fits = [
            [
                (here[axis] + step < sizes[axis]) if way > 0 else (here[axis] >= step)
                for step in range(sizes[axis])
            ]
            for axis in range(3)
        ]
        for offset in offsets:
            core, y, x = (here[axis] + way * offset[axis] for axis in range(3))

            @pl.when(all_of([fits[axis][offset[axis]] for axis in range(3) if offset[axis]]))
            def _():
                pl.semaphore_signal(
                    semaphore,
                    inc=1,
                    device_id=(slab, y * cores + cores - 1 - core, x),
                    device_id_type=MESH,
                )


    def all_of(conditions):
        return functools.reduce(jnp.logical_and, conditions)

    def same(spot):
        return all_of([a == b for a, b in zip(spot, here)])

    def after_me(spot):
        return jnp.logical_and(
            all_of([a >= b for a, b in zip(spot, here)]), jnp.logical_not(same(spot))
        )

    def before_me(spot):
        return jnp.logical_and(
            all_of([a <= b for a, b in zip(spot, here)]), jnp.logical_not(same(spot))
        )

    def load_state(z):
        return pltpu.make_async_copy(state.at[:, :, z], modes.at[:, :, z], state_sem.at[z])

    def load_labels(z):
        return pltpu.make_async_copy(shells.at[z], labels.at[z], label_sem.at[z])

    def group_peer(step):
        peer = lax.rem(me + step, group)
        return (peer, peer // px_count, lax.rem(peer, px_count))

    def slab_peer(step):
        return lax.rem(slab + step, slab_count)

    def block(source, dest_py, dest_px):
        return source.at[
            :,
            :,
            pl.ds(dest_py * planes_out, planes_out),
            :,
            pl.ds(pl.multiple_of(dest_px * columns_out, columns_out), columns_out),
        ]

    def strip(buffer, source):
        return buffer.at[:, :, :, pl.ds(pl.multiple_of(source * rows, rows), rows), :]

    def send_block(dest_py, dest_px):
        return pltpu.make_async_remote_copy(
            src_ref=block(state, dest_py, dest_px),
            dst_ref=strip(moved, me),
            send_sem=send_sem.at[dest_py * px_count + dest_px],
            recv_sem=recv_sem.at[me],
            device_id=(slab, dest_py, dest_px),
            device_id_type=MESH,
        )

    def take_block(source, source_py, source_px):
        return pltpu.make_async_remote_copy(
            src_ref=block(state, source_py, source_px),
            dst_ref=strip(moved, source),
            send_sem=send_sem.at[source],
            recv_sem=recv_sem.at[source],
            device_id=(slab, source_py, source_px),
            device_id_type=MESH,
        )

    def slab_copy(dest, slot):
        return pltpu.make_async_remote_copy(
            src_ref=slab_parts.at[slab],
            dst_ref=slab_parts.at[slot],
            send_sem=slab_send.at[dest],
            recv_sem=slab_recv.at[slot],
            device_id=(dest, py, px),
            device_id_type=MESH,
        )

    def part_copy(dest, dest_py, dest_px, slot):
        return pltpu.make_async_remote_copy(
            src_ref=group_parts.at[me],
            dst_ref=group_parts.at[slot],
            send_sem=part_send.at[dest],
            recv_sem=part_recv.at[slot],
            device_id=(slab, dest_py, dest_px),
            device_id_type=MESH,
        )

    barrier = pltpu.get_barrier_semaphore()
    tell_all(1, barrier)

    for q_slab in range(1, slab_count):

        @pl.when(q_slab > slab)
        def _():
            pl.semaphore_signal(
                barrier, inc=1, device_id=(q_slab, py, px), device_id_type=MESH
            )

    before = (here[0] + 1) * (here[1] + 1) * (here[2] + 1) - 1 + slab

    @pl.when(before > 0)
    def _():
        pl.semaphore_wait(barrier, before)

    def spot_of(dest_py, dest_px):
        return (cores - 1 - lax.rem(dest_py, cores), dest_py // cores, dest_px)

    def late(dest_py, dest_px):
        return is_late(py_count, px_count, py, px, dest_py, dest_px)

    def send_if(condition, dest_py, dest_px):
        @pl.when(jnp.logical_and(condition, jnp.logical_not(late(dest_py, dest_px))))
        def _():
            send_block(dest_py, dest_px).start()

    def send_at(distance, wanted, turns=range(py_count)):
        for turn in turns:
            dest_py = lax.rem(py + turn, py_count)
            for dest_px in (px + distance, px - distance):
                inside = jnp.logical_and(dest_px >= 0, dest_px < px_count)
                send_if(
                    jnp.logical_and(inside, wanted(dest_py, dest_px)), dest_py, dest_px
                )

    def send_far(wanted):
        for distance in range(px_count - 1, 1, -1):
            send_at(distance, wanted)

    next_py = py + cores - 1 - 2 * lax.rem(py, cores)

    def is_next(q_py, q_px):
        return all_of([q_py == next_py, q_px == px + 1, q_px == px_count // 2])

    def is_outward(q_py, q_px):
        same_side = (q_px < px_count // 2) == (px < px_count // 2)
        return jnp.logical_and(inner_at(px, px_count), same_side)

    def send_near():
        apart = [turn for turn in range(py_count) if turn % cores]
        alike = [turn for turn in range(py_count) if turn % cores == 0]
        send_at(
            1,
            lambda *dest: jnp.logical_not(
                jnp.logical_or(is_next(*dest), is_outward(*dest))
            ),
            apart + alike,
        )

    def hear(rise_y, rise_px):
        for core in range(cores):
            spot = (core, here[1] + rise_y, px + rise_px)
            q_py = spot[1] * cores + cores - 1 - core
            exists = jnp.logical_and(q_py < py_count, spot[2] < px_count)

            @pl.when(jnp.logical_and(exists, after_me(spot)))
            def _():
                pl.semaphore_wait(ready_sem.at[q_py * px_count + spot[2]], 1)

    tell_all(-1, ready_sem.at[me])

    send_far(lambda *dest: before_me(spot_of(*dest)))

    for q_slab in range(slab_count - 1):

        @pl.when(q_slab < slab)
        def _():
            pl.semaphore_signal(
                slab_ready.at[slab], inc=1, device_id=(q_slab, py, px), device_id_type=MESH
            )

    rises = [(y, x) for y in range(py_count // cores) for x in range(px_count)]
    for rise_y, rise_px in sorted(rises, key=lambda rise: (sum(rise), rise[0])):
        hear(rise_y, rise_px)

        def reached(dest_py, dest_px):
            return all_of(
                [
                    jnp.maximum(dest_py // cores - here[1], 0) == rise_y,
                    jnp.maximum(dest_px - px, 0) == rise_px,
                    jnp.logical_not(before_me(spot_of(dest_py, dest_px))),
                ]
            )

        if rise_px == 1 and rise_y == 0:
            send_if(is_next(next_py, px + 1), next_py, px + 1)
        send_far(reached)

    send_at(1, is_outward)
    for turn in range(1, py_count):
        send_block(lax.rem(py + turn, py_count), px).start()

    for z in range(planes):
        load_state(z).start()
        load_labels(z).start()

    low_ids = lax.broadcasted_iota(jnp.int32, (LOW, columns), 0)
    high_ids = lax.broadcasted_iota(jnp.int32, (HIGH, columns), 0)

    def add_rows(z, start, running):
        values = modes[:, :, z, pl.ds(start, GROUP_ROWS), :].astype(jnp.float32)
        energy = 0.5 * jnp.sum(values * values, axis=(0, 1))
        upper = energy.astype(jnp.bfloat16).astype(jnp.float32)
        lower = energy - upper
        numbers = labels[z, pl.ds(start, GROUP_ROWS), :]
        high = numbers >> (LOW.bit_length() - 1)
        low = numbers & (LOW - 1)
        for row in range(GROUP_ROWS):
            one = slice(row, row + 1)
            hot = high_ids == high[one]
            weighted = jnp.concatenate(
                [jnp.where(hot, upper[one], 0.0), jnp.where(hot, lower[one], 0.0)], axis=0
            ).astype(jnp.bfloat16)
            onehot = jnp.where(low_ids == low[one], 1.0, 0.0).astype(jnp.bfloat16)
            running = running + lax.dot_general(
                weighted, onehot, (((1,), (1,)), ((), ())), preferred_element_type=jnp.float32
            )
        return running

    running = jnp.zeros((2 * HIGH, LOW), jnp.float32)
    for z in range(planes):
        load_state(z).wait()
        load_labels(z).wait()

    groups = rows // GROUP_ROWS
    running = lax.fori_loop(
        0,
        planes * groups,
        lambda i, total: add_rows(
            i // groups, pl.multiple_of(lax.rem(i, groups) * GROUP_ROWS, GROUP_ROWS), total
        ),
        running,
    )
    part = running[:HIGH] + running[HIGH:]
    per_row = LANES // LOW
    for high in range(HIGH):
        lane = (high % per_row) * LOW
        slab_parts[slab, high // per_row : high // per_row + 1, lane : lane + LOW] = part[
            high : high + 1
        ]

    for q_slab in range(1, slab_count):

        @pl.when(q_slab > slab)
        def _():
            pl.semaphore_wait(slab_ready.at[q_slab], 1)

    for step in range(1, slab_count):
        slab_copy(slab_peer(step), slab).start()
    for step in range(1, slab_count):
        slab_copy(slab_peer(step), slab_peer(step)).wait_recv()
    total = slab_parts[0]
    for slot in range(1, slab_count):
        total = total + slab_parts[slot]
    group_parts[me] = total
    for step in range(1, group):
        part_copy(*group_peer(step), me).start()

    send_near()

    def widen(source, target):
        for real in range(source.shape[0]):
            for part_of in range(source.shape[1]):
                for plane in range(source.shape[2]):
                    target[real, part_of, plane] = source[real, part_of, plane].astype(
                        jnp.float32
                    )

    widen(block(modes, py, px), strip(out, me))

    for step in range(1, group):
        peer, peer_py, peer_px = group_peer(step)
        part_copy(peer, peer_py, peer_px, peer).wait_recv()
    total = group_parts[0]
    for slot in range(1, group):
        total = total + group_parts[slot]
    modes_all = planes * rows * columns * slab_count * group
    spec[...] = total * (SHELLS / modes_all)

    def take_and_widen(source_py, source_px):
        source = source_py * px_count + source_px
        take_block(source, source_py, source_px).wait_recv()
        widen(strip(moved, source), strip(out, source))

    for step in range(1, slab_count):
        slab_copy(slab_peer(step), slab).wait_send()
    for step in range(1, group):
        peer, peer_py, peer_px = group_peer(step)
        part_copy(peer, peer_py, peer_px, me).wait_send()

    half = px_count // 2
    ahead = jnp.where(px < half, 1, px_count - 1)

    def take_step(step, carry):
        source_px = lax.rem(px + ahead * (half + step // py_count), px_count)
        source_py = lax.rem(py + py_count - lax.rem(step, py_count), py_count)

        other = jnp.logical_or(source_px != px, source_py != py)
        here_now = jnp.logical_not(late(source_py, source_px))

        @pl.when(jnp.logical_and(other, here_now))
        def _():
            take_and_widen(source_py, source_px)

        return carry

    lax.fori_loop(0, group, take_step, 0)
    for step in range(1, group):
        _, peer_py, peer_px = group_peer(step)

        @pl.when(jnp.logical_not(late(peer_py, peer_px)))
        def _():
            send_block(peer_py, peer_px).wait_send()


def run_copies(copies, sems):
    def each(act):
        for i, (condition, source, target) in enumerate(copies):
            copy = pltpu.make_async_copy(source, target, sems.at[i])
            if condition is None:
                act(copy)
            else:
                pl.when(condition)(functools.partial(act, copy))

    each(lambda copy: copy.start())
    each(lambda copy: copy.wait())


def store_kernel(py_count, px_count, widened, totals, out, spectrum, sems):
    py = lax.axis_index("py")
    px = lax.axis_index("px")
    rows = out.shape[3] // (py_count * px_count)
    copies = [(None, totals, spectrum)]
    for source_py in range(py_count):
        for source_px in range(px_count):
            start = (source_py * px_count + source_px) * rows
            strip = (slice(None), slice(None), slice(None), pl.ds(start, rows))
            missing = is_late(py_count, px_count, py, px, source_py, source_px)
            copies.append((jnp.logical_not(missing), widened.at[strip], out.at[strip]))
    run_copies(copies, sems)


def rest_kernel(py_count, px_count, rest, stored, out, sems):
    py = lax.axis_index("py")
    px = lax.axis_index("px")
    cores = core_count(py_count)
    rows = rest.shape[4]
    mate = across(px, px_count)
    copies = []
    for chip in range(py_count // cores):
        start = pl.multiple_of(((chip * cores + cores - 1) * px_count + mate) * rows, rows)
        copies.append(
            (
                is_late(py_count, px_count, py, px, chip * cores + cores - 1, mate),
                rest.at[chip],
                out.at[:, :, :, pl.ds(start, rows)],
            )
        )
    run_copies(copies, sems)


def local(state, shells):
    slab_count = lax.axis_size("slab")
    py_count = lax.axis_size("py")
    px_count = lax.axis_size("px")
    group = py_count * px_count
    _, _, planes, rows, columns = state.shape
    moved_shape = (2, 3, planes // py_count, rows * group, columns // px_count)
    widened, totals = pl.pallas_call(
        functools.partial(move_kernel, slab_count, py_count, px_count),
        out_shape=(
            pltpu.VMEM(moved_shape, jnp.float32),
            pltpu.VMEM((SPEC_ROWS, LANES), jnp.float32),
        ),
        in_specs=[pl.BlockSpec(memory_space=pl.ANY)] * 2,
        out_specs=(
            pl.BlockSpec(memory_space=pltpu.VMEM),
            pl.BlockSpec(memory_space=pltpu.VMEM),
        ),
        scratch_shapes=[
            pltpu.VMEM(moved_shape, state.dtype),
            pltpu.VMEM(state.shape, state.dtype),
            pltpu.VMEM(shells.shape, shells.dtype),
            pltpu.VMEM((slab_count, SPEC_ROWS, LANES), jnp.float32),
            pltpu.VMEM((group, SPEC_ROWS, LANES), jnp.float32),
            pltpu.SemaphoreType.DMA((planes,)),
            pltpu.SemaphoreType.DMA((planes,)),
            pltpu.SemaphoreType.DMA((group,)),
            pltpu.SemaphoreType.DMA((group,)),
            pltpu.SemaphoreType.DMA((slab_count,)),
            pltpu.SemaphoreType.DMA((slab_count,)),
            pltpu.SemaphoreType.DMA((group,)),
            pltpu.SemaphoreType.DMA((group,)),
            pltpu.SemaphoreType.REGULAR((group,)),
            pltpu.SemaphoreType.REGULAR((slab_count,)),
        ],
        name="move",
        compiler_params=pltpu.CompilerParams(
            collective_id=0, has_side_effects=True, vmem_limit_bytes=40 << 20
        ),
    )(
        pltpu.with_memory_space_constraint(state, pltpu.HBM),
        pltpu.with_memory_space_constraint(shells, pltpu.HBM),
    )
    anywhere = pl.BlockSpec(memory_space=pl.ANY)
    in_vmem = pl.BlockSpec(memory_space=pltpu.VMEM)
    stored, spectrum = pl.pallas_call(
        functools.partial(store_kernel, py_count, px_count),
        out_shape=(
            jax.ShapeDtypeStruct(moved_shape, jnp.float32),
            jax.ShapeDtypeStruct((SPEC_ROWS, LANES), jnp.float32),
        ),
        in_specs=[in_vmem] * 2,
        out_specs=(anywhere, anywhere),
        scratch_shapes=[pltpu.SemaphoreType.DMA((1 + group,))],
        name="store",
        compiler_params=pltpu.CompilerParams(vmem_limit_bytes=40 << 20),
    )(widened, totals)
    chips = py_count // core_count(py_count)
    rest_shape = (chips, 2, 3, planes // py_count, rows, columns // px_count)
    rest = pl.pallas_call(
        functools.partial(swap_kernel, py_count, px_count),
        out_shape=pltpu.VMEM(rest_shape, jnp.float32),
        in_specs=[anywhere] * 2,
        out_specs=in_vmem,
        scratch_shapes=[
            pltpu.VMEM(rest_shape, state.dtype),
            pltpu.SemaphoreType.DMA((chips,)),
            pltpu.SemaphoreType.DMA((chips,)),
        ],
        name="swap",
        compiler_params=pltpu.CompilerParams(
            collective_id=1, has_side_effects=True, vmem_limit_bytes=40 << 20
        ),
    )(
        pltpu.with_memory_space_constraint(state, pltpu.HBM),
        pltpu.with_memory_space_constraint(spectrum, pltpu.HBM),
    )
    restored = pl.pallas_call(
        functools.partial(rest_kernel, py_count, px_count),
        out_shape=jax.ShapeDtypeStruct(moved_shape, jnp.float32),
        in_specs=[in_vmem, anywhere],
        out_specs=anywhere,
        scratch_shapes=[pltpu.SemaphoreType.DMA((chips,))],
        input_output_aliases={1: 0},
        name="store_rest",
        compiler_params=pltpu.CompilerParams(vmem_limit_bytes=40 << 20),
    )(rest, stored)
    return (restored, spectrum.reshape(SHELLS))


def solution(mesh):
    return jax.shard_map(
        local,
        mesh=mesh,
        in_specs=(P(None, None, "slab", ("py", "px"), None), P("slab", ("py", "px"), None)),
        out_specs=(P(None, None, ("slab", "py"), None, "px"), P()),
        check_vma=False,
    )
```

```python
import functools

import jax
import jax.numpy as jnp
from jax import lax
from jax.experimental import pallas as pl
from jax.experimental.pallas import tpu as pltpu
from jax.sharding import PartitionSpec as P

SHELLS = 512
LOW = 32
HIGH = SHELLS // LOW
LANES = 128
SPEC_ROWS = SHELLS // LANES
GROUP_ROWS = 16
CORES = 2
MESH = pl.DeviceIdType.MESH


def core_count(py_count):
    return CORES if py_count % CORES == 0 else 1


def inner_at(px, px_count):
    half = px_count // 2
    return jnp.logical_and(half > 0, jnp.logical_or(px == half - 1, px == half))


def across(px, px_count):
    return 2 * (px_count // 2) - 1 - px


def is_late(py_count, px_count, py, px, dest_py, dest_px):
    cores = core_count(py_count)
    lasts = jnp.logical_and(lax.rem(py, cores) == cores - 1, lax.rem(dest_py, cores) == cores - 1)
    mates = jnp.logical_and(inner_at(px, px_count), dest_px == across(px, px_count))
    return jnp.logical_and(cores > 1, jnp.logical_and(lasts, mates))


def swap_kernel(py_count, px_count, state, after, rest, moved, send_sem, recv_sem):
    slab = lax.axis_index("slab")
    py = lax.axis_index("py")
    px = lax.axis_index("px")
    cores = core_count(py_count)
    chips = py_count // cores
    _, _, planes, rows, columns = state.shape
    planes_out = planes // py_count
    columns_out = columns // px_count
    mate = across(px, px_count)

    def copy(chip, slot):
        return pltpu.make_async_remote_copy(
            src_ref=state.at[
                :,
                :,
                pl.ds((chip * cores + cores - 1) * planes_out, planes_out),
                :,
                pl.ds(pl.multiple_of(mate * columns_out, columns_out), columns_out),
            ],
            dst_ref=moved.at[slot],
            send_sem=send_sem.at[chip],
            recv_sem=recv_sem.at[slot],
            device_id=(slab, chip * cores + cores - 1, mate),
            device_id_type=MESH,
        )

    @pl.when(is_late(py_count, px_count, py, px, cores - 1, mate))
    def _():
        here = py // cores
        barrier = pltpu.get_barrier_semaphore()
        for chip in range(chips):
            pl.semaphore_signal(
                barrier, inc=1, device_id=(slab, chip * cores + cores - 1, mate), device_id_type=MESH
            )
        pl.semaphore_wait(barrier, chips)
        for turn in range(chips):
            copy(turn, here).start()
        for turn in range(chips):
            chip = lax.rem(here + chips - turn, chips)
            copy(chip, chip).wait_recv()
            for real in range(moved.shape[1]):
                for part in range(moved.shape[2]):
                    for plane in range(planes_out):
                        piece = (chip, real, part, plane)
                        rest[piece] = moved[piece].astype(jnp.float32)
        for chip in range(chips):
            copy(chip, here).wait_send()


def move_kernel(
    slab_count,
    py_count,
    px_count,
    state,
    shells,
    out,
    spec,
    moved,
    modes,
    labels,
    slab_parts,
    group_parts,
    state_sem,
    label_sem,
    send_sem,
    recv_sem,
    slab_send,
    slab_recv,
    part_send,
    part_recv,
    ready_sem,
    slab_ready,
):
    slab = lax.axis_index("slab")
    py = lax.axis_index("py")
    px = lax.axis_index("px")
    group = py_count * px_count
    me = py * px_count + px
    cores = core_count(py_count)
    _, _, planes, rows, columns = state.shape
    planes_out = planes // py_count
    columns_out = columns // px_count

    def position(any_py, any_px):
        return (cores - 1 - any_py % cores, any_py // cores, any_px)

    here = (cores - 1 - lax.rem(py, cores), py // cores, px)
    sizes = (cores, py_count // cores, px_count)
    offsets = sorted(
        (
            (core, y, x)
            for core in range(sizes[0])
            for y in range(sizes[1])
            for x in range(sizes[2])
            if core + y + x > 0
        ),
        key=lambda offset: (offset[1] + offset[2], offset[1], offset[0]),
    )

    def tell_all(way, semaphore):
        fits = [
            [
                (here[axis] + step < sizes[axis]) if way > 0 else (here[axis] >= step)
                for step in range(sizes[axis])
            ]
            for axis in range(3)
        ]
        for offset in offsets:
            core, y, x = (here[axis] + way * offset[axis] for axis in range(3))

            @pl.when(all_of([fits[axis][offset[axis]] for axis in range(3) if offset[axis]]))
            def _():
                pl.semaphore_signal(
                    semaphore,
                    inc=1,
                    device_id=(slab, y * cores + cores - 1 - core, x),
                    device_id_type=MESH,
                )


    def all_of(conditions):
        return functools.reduce(jnp.logical_and, conditions)

    def same(spot):
        return all_of([a == b for a, b in zip(spot, here)])

    def after_me(spot):
        return jnp.logical_and(
            all_of([a >= b for a, b in zip(spot, here)]), jnp.logical_not(same(spot))
        )

    def before_me(spot):
        return jnp.logical_and(
            all_of([a <= b for a, b in zip(spot, here)]), jnp.logical_not(same(spot))
        )

    def load_state(z):
        return pltpu.make_async_copy(state.at[:, :, z], modes.at[:, :, z], state_sem.at[z])

    def load_labels(z):
        return pltpu.make_async_copy(shells.at[z], labels.at[z], label_sem.at[z])

    def group_peer(step):
        peer = lax.rem(me + step, group)
        return (peer, peer // px_count, lax.rem(peer, px_count))

    def slab_peer(step):
        return lax.rem(slab + step, slab_count)

    def block(source, dest_py, dest_px):
        return source.at[
            :,
            :,
            pl.ds(dest_py * planes_out, planes_out),
            :,
            pl.ds(pl.multiple_of(dest_px * columns_out, columns_out), columns_out),
        ]

    def strip(buffer, source):
        return buffer.at[:, :, :, pl.ds(pl.multiple_of(source * rows, rows), rows), :]

    def send_block(dest_py, dest_px, source=state):
        return pltpu.make_async_remote_copy(
            src_ref=block(source, dest_py, dest_px),
            dst_ref=strip(moved, me),
            send_sem=send_sem.at[dest_py * px_count + dest_px],
            recv_sem=recv_sem.at[me],
            device_id=(slab, dest_py, dest_px),
            device_id_type=MESH,
        )

    def take_block(source, source_py, source_px):
        return pltpu.make_async_remote_copy(
            src_ref=block(state, source_py, source_px),
            dst_ref=strip(moved, source),
            send_sem=send_sem.at[source],
            recv_sem=recv_sem.at[source],
            device_id=(slab, source_py, source_px),
            device_id_type=MESH,
        )

    def slab_copy(dest, slot):
        return pltpu.make_async_remote_copy(
            src_ref=slab_parts.at[slab],
            dst_ref=slab_parts.at[slot],
            send_sem=slab_send.at[dest],
            recv_sem=slab_recv.at[slot],
            device_id=(dest, py, px),
            device_id_type=MESH,
        )

    def part_copy(dest, dest_py, dest_px, slot):
        return pltpu.make_async_remote_copy(
            src_ref=group_parts.at[me],
            dst_ref=group_parts.at[slot],
            send_sem=part_send.at[dest],
            recv_sem=part_recv.at[slot],
            device_id=(slab, dest_py, dest_px),
            device_id_type=MESH,
        )

    barrier = pltpu.get_barrier_semaphore()
    tell_all(1, barrier)

    for q_slab in range(1, slab_count):

        @pl.when(q_slab > slab)
        def _():
            pl.semaphore_signal(
                barrier, inc=1, device_id=(q_slab, py, px), device_id_type=MESH
            )

    before = (here[0] + 1) * (here[1] + 1) * (here[2] + 1) - 1 + slab

    @pl.when(before > 0)
    def _():
        pl.semaphore_wait(barrier, before)

    def spot_of(dest_py, dest_px):
        return (cores - 1 - lax.rem(dest_py, cores), dest_py // cores, dest_px)

    def late(dest_py, dest_px):
        return is_late(py_count, px_count, py, px, dest_py, dest_px)

    def send_if(condition, dest_py, dest_px, source=state):
        @pl.when(jnp.logical_and(condition, jnp.logical_not(late(dest_py, dest_px))))
        def _():
            send_block(dest_py, dest_px, source).start()

    def send_at(distance, wanted, turns=range(py_count), source=state):
        for turn in turns:
            dest_py = lax.rem(py + turn, py_count)
            for dest_px in (px + distance, px - distance):
                inside = jnp.logical_and(dest_px >= 0, dest_px < px_count)
                send_if(
                    jnp.logical_and(inside, wanted(dest_py, dest_px)),
                    dest_py,
                    dest_px,
                    source,
                )

    def send_far(wanted):
        for distance in range(px_count - 1, 1, -1):
            send_at(distance, wanted)

    next_py = py + cores - 1 - 2 * lax.rem(py, cores)

    def is_next(q_py, q_px):
        return all_of([q_py == next_py, q_px == px + 1, q_px == px_count // 2])

    def is_outward(q_py, q_px):
        same_side = (q_px < px_count // 2) == (px < px_count // 2)
        return jnp.logical_and(inner_at(px, px_count), same_side)

    def send_near():
        apart = [turn for turn in range(py_count) if turn % cores]
        alike = [turn for turn in range(py_count) if turn % cores == 0]
        send_at(
            1,
            lambda *dest: jnp.logical_not(
                jnp.logical_or(is_next(*dest), is_outward(*dest))
            ),
            apart + alike,
            modes,
        )

    def hear(rise_y, rise_px):
        for core in range(cores):
            spot = (core, here[1] + rise_y, px + rise_px)
            q_py = spot[1] * cores + cores - 1 - core
            exists = jnp.logical_and(q_py < py_count, spot[2] < px_count)

            @pl.when(jnp.logical_and(exists, after_me(spot)))
            def _():
                pl.semaphore_wait(ready_sem.at[q_py * px_count + spot[2]], 1)

    tell_all(-1, ready_sem.at[me])

    send_far(lambda *dest: before_me(spot_of(*dest)))

    for q_slab in range(slab_count - 1):

        @pl.when(q_slab < slab)
        def _():
            pl.semaphore_signal(
                slab_ready.at[slab], inc=1, device_id=(q_slab, py, px), device_id_type=MESH
            )

    rises = [(y, x) for y in range(py_count // cores) for x in range(px_count)]
    for rise_y, rise_px in sorted(rises, key=lambda rise: (sum(rise), rise[0])):
        hear(rise_y, rise_px)

        def reached(dest_py, dest_px):
            return all_of(
                [
                    jnp.maximum(dest_py // cores - here[1], 0) == rise_y,
                    jnp.maximum(dest_px - px, 0) == rise_px,
                    jnp.logical_not(before_me(spot_of(dest_py, dest_px))),
                ]
            )

        if rise_px == 1 and rise_y == 0:
            send_if(is_next(next_py, px + 1), next_py, px + 1)
        send_far(reached)

    send_at(1, is_outward)
    for turn in range(1, py_count):
        send_block(lax.rem(py + turn, py_count), px).start()

    for z in range(planes):
        load_state(z).start()
        load_labels(z).start()

    low_ids = lax.broadcasted_iota(jnp.int32, (LOW, columns), 0)
    high_ids = lax.broadcasted_iota(jnp.int32, (HIGH, columns), 0)

    def add_rows(z, start, running):
        values = modes[:, :, z, pl.ds(start, GROUP_ROWS), :].astype(jnp.float32)
        energy = 0.5 * jnp.sum(values * values, axis=(0, 1))
        upper = energy.astype(jnp.bfloat16).astype(jnp.float32)
        lower = energy - upper
        numbers = labels[z, pl.ds(start, GROUP_ROWS), :]
        high = numbers >> (LOW.bit_length() - 1)
        low = numbers & (LOW - 1)
        for row in range(GROUP_ROWS):
            one = slice(row, row + 1)
            hot = high_ids == high[one]
            weighted = jnp.concatenate(
                [jnp.where(hot, upper[one], 0.0), jnp.where(hot, lower[one], 0.0)], axis=0
            ).astype(jnp.bfloat16)
            onehot = jnp.where(low_ids == low[one], 1.0, 0.0).astype(jnp.bfloat16)
            running = running + lax.dot_general(
                weighted, onehot, (((1,), (1,)), ((), ())), preferred_element_type=jnp.float32
            )
        return running

    running = jnp.zeros((2 * HIGH, LOW), jnp.float32)
    for z in range(planes):
        load_state(z).wait()
        load_labels(z).wait()

    groups = rows // GROUP_ROWS
    running = lax.fori_loop(
        0,
        planes * groups,
        lambda i, total: add_rows(
            i // groups, pl.multiple_of(lax.rem(i, groups) * GROUP_ROWS, GROUP_ROWS), total
        ),
        running,
    )
    part = running[:HIGH] + running[HIGH:]
    per_row = LANES // LOW
    for high in range(HIGH):
        lane = (high % per_row) * LOW
        slab_parts[slab, high // per_row : high // per_row + 1, lane : lane + LOW] = part[
            high : high + 1
        ]

    for q_slab in range(1, slab_count):

        @pl.when(q_slab > slab)
        def _():
            pl.semaphore_wait(slab_ready.at[q_slab], 1)

    for step in range(1, slab_count):
        slab_copy(slab_peer(step), slab).start()
    for step in range(1, slab_count):
        slab_copy(slab_peer(step), slab_peer(step)).wait_recv()
    total = slab_parts[0]
    for slot in range(1, slab_count):
        total = total + slab_parts[slot]
    group_parts[me] = total
    for step in range(1, group):
        part_copy(*group_peer(step), me).start()

    send_near()

    def widen(source, target):
        for real in range(source.shape[0]):
            for part_of in range(source.shape[1]):
                for plane in range(source.shape[2]):
                    target[real, part_of, plane] = source[real, part_of, plane].astype(
                        jnp.float32
                    )

    widen(block(modes, py, px), strip(out, me))

    for step in range(1, group):
        peer, peer_py, peer_px = group_peer(step)
        part_copy(peer, peer_py, peer_px, peer).wait_recv()
    total = group_parts[0]
    for slot in range(1, group):
        total = total + group_parts[slot]
    modes_all = planes * rows * columns * slab_count * group
    spec[...] = total * (SHELLS / modes_all)

    def take_and_widen(source_py, source_px):
        source = source_py * px_count + source_px
        take_block(source, source_py, source_px).wait_recv()
        widen(strip(moved, source), strip(out, source))

    for step in range(1, slab_count):
        slab_copy(slab_peer(step), slab).wait_send()
    for step in range(1, group):
        peer, peer_py, peer_px = group_peer(step)
        part_copy(peer, peer_py, peer_px, me).wait_send()

    half = px_count // 2
    ahead = jnp.where(px < half, 1, px_count - 1)

    def take_step(step, carry):
        source_px = lax.rem(px + ahead * (half + step // py_count), px_count)
        source_py = lax.rem(py + py_count - lax.rem(step, py_count), py_count)

        other = jnp.logical_or(source_px != px, source_py != py)
        here_now = jnp.logical_not(late(source_py, source_px))

        @pl.when(jnp.logical_and(other, here_now))
        def _():
            take_and_widen(source_py, source_px)

        return carry

    lax.fori_loop(0, group, take_step, 0)
    for step in range(1, group):
        _, peer_py, peer_px = group_peer(step)

        @pl.when(jnp.logical_not(late(peer_py, peer_px)))
        def _():
            send_block(peer_py, peer_px).wait_send()


def run_copies(copies, sems):
    def each(act):
        for i, (condition, source, target) in enumerate(copies):
            copy = pltpu.make_async_copy(source, target, sems.at[i])
            if condition is None:
                act(copy)
            else:
                pl.when(condition)(functools.partial(act, copy))

    each(lambda copy: copy.start())
    each(lambda copy: copy.wait())


def store_kernel(py_count, px_count, widened, totals, out, spectrum, sems):
    py = lax.axis_index("py")
    px = lax.axis_index("px")
    rows = out.shape[3] // (py_count * px_count)
    copies = [(None, totals, spectrum)]
    for source_py in range(py_count):
        for source_px in range(px_count):
            start = (source_py * px_count + source_px) * rows
            strip = (slice(None), slice(None), slice(None), pl.ds(start, rows))
            missing = is_late(py_count, px_count, py, px, source_py, source_px)
            copies.append((jnp.logical_not(missing), widened.at[strip], out.at[strip]))
    run_copies(copies, sems)


def rest_kernel(py_count, px_count, rest, stored, out, sems):
    py = lax.axis_index("py")
    px = lax.axis_index("px")
    cores = core_count(py_count)
    rows = rest.shape[4]
    mate = across(px, px_count)
    copies = []
    for chip in range(py_count // cores):
        start = pl.multiple_of(((chip * cores + cores - 1) * px_count + mate) * rows, rows)
        copies.append(
            (
                is_late(py_count, px_count, py, px, chip * cores + cores - 1, mate),
                rest.at[chip],
                out.at[:, :, :, pl.ds(start, rows)],
            )
        )
    run_copies(copies, sems)


def local(state, shells):
    slab_count = lax.axis_size("slab")
    py_count = lax.axis_size("py")
    px_count = lax.axis_size("px")
    group = py_count * px_count
    _, _, planes, rows, columns = state.shape
    moved_shape = (2, 3, planes // py_count, rows * group, columns // px_count)
    widened, totals = pl.pallas_call(
        functools.partial(move_kernel, slab_count, py_count, px_count),
        out_shape=(
            pltpu.VMEM(moved_shape, jnp.float32),
            pltpu.VMEM((SPEC_ROWS, LANES), jnp.float32),
        ),
        in_specs=[pl.BlockSpec(memory_space=pl.ANY)] * 2,
        out_specs=(
            pl.BlockSpec(memory_space=pltpu.VMEM),
            pl.BlockSpec(memory_space=pltpu.VMEM),
        ),
        scratch_shapes=[
            pltpu.VMEM(moved_shape, state.dtype),
            pltpu.VMEM(state.shape, state.dtype),
            pltpu.VMEM(shells.shape, shells.dtype),
            pltpu.VMEM((slab_count, SPEC_ROWS, LANES), jnp.float32),
            pltpu.VMEM((group, SPEC_ROWS, LANES), jnp.float32),
            pltpu.SemaphoreType.DMA((planes,)),
            pltpu.SemaphoreType.DMA((planes,)),
            pltpu.SemaphoreType.DMA((group,)),
            pltpu.SemaphoreType.DMA((group,)),
            pltpu.SemaphoreType.DMA((slab_count,)),
            pltpu.SemaphoreType.DMA((slab_count,)),
            pltpu.SemaphoreType.DMA((group,)),
            pltpu.SemaphoreType.DMA((group,)),
            pltpu.SemaphoreType.REGULAR((group,)),
            pltpu.SemaphoreType.REGULAR((slab_count,)),
        ],
        name="move",
        compiler_params=pltpu.CompilerParams(
            collective_id=0, has_side_effects=True, vmem_limit_bytes=40 << 20
        ),
    )(
        pltpu.with_memory_space_constraint(state, pltpu.HBM),
        pltpu.with_memory_space_constraint(shells, pltpu.HBM),
    )
    anywhere = pl.BlockSpec(memory_space=pl.ANY)
    in_vmem = pl.BlockSpec(memory_space=pltpu.VMEM)
    stored, spectrum = pl.pallas_call(
        functools.partial(store_kernel, py_count, px_count),
        out_shape=(
            jax.ShapeDtypeStruct(moved_shape, jnp.float32),
            jax.ShapeDtypeStruct((SPEC_ROWS, LANES), jnp.float32),
        ),
        in_specs=[in_vmem] * 2,
        out_specs=(anywhere, anywhere),
        scratch_shapes=[pltpu.SemaphoreType.DMA((1 + group,))],
        name="store",
        compiler_params=pltpu.CompilerParams(vmem_limit_bytes=40 << 20),
    )(widened, totals)
    chips = py_count // core_count(py_count)
    rest_shape = (chips, 2, 3, planes // py_count, rows, columns // px_count)
    rest = pl.pallas_call(
        functools.partial(swap_kernel, py_count, px_count),
        out_shape=pltpu.VMEM(rest_shape, jnp.float32),
        in_specs=[anywhere] * 2,
        out_specs=in_vmem,
        scratch_shapes=[
            pltpu.VMEM(rest_shape, state.dtype),
            pltpu.SemaphoreType.DMA((chips,)),
            pltpu.SemaphoreType.DMA((chips,)),
        ],
        name="swap",
        compiler_params=pltpu.CompilerParams(
            collective_id=1, has_side_effects=True, vmem_limit_bytes=40 << 20
        ),
    )(
        pltpu.with_memory_space_constraint(state, pltpu.HBM),
        pltpu.with_memory_space_constraint(spectrum, pltpu.HBM),
    )
    restored = pl.pallas_call(
        functools.partial(rest_kernel, py_count, px_count),
        out_shape=jax.ShapeDtypeStruct(moved_shape, jnp.float32),
        in_specs=[in_vmem, anywhere],
        out_specs=anywhere,
        scratch_shapes=[pltpu.SemaphoreType.DMA((chips,))],
        input_output_aliases={1: 0},
        name="store_rest",
        compiler_params=pltpu.CompilerParams(vmem_limit_bytes=40 << 20),
    )(rest, stored)
    return (restored, spectrum.reshape(SHELLS))


def solution(mesh):
    return jax.shard_map(
        local,
        mesh=mesh,
        in_specs=(P(None, None, "slab", ("py", "px"), None), P("slab", ("py", "px"), None)),
        out_specs=(P(None, None, ("slab", "py"), None, "px"), P()),
        check_vma=False,
    )
```
